256 devices in a mesh: sector: 16 (over z, core), term: 16 (over y, x).
Axes of the slice: x: 4, y: 4, z: 8, core: 2. Of those that a mesh axis runs over, the one named last changes fastest.
Arguments:
- psi: bfloat16 [256, 256, 256], P('sector'), may hold values from -6 to 6
- sector_sizes: int32 [256], P('sector'), may hold values from 64 to 256, as said below
- left_env: bfloat16 [768, 16, 256, 256], P('term', 'sector'), may hold values from -0.0546875 to 0.0546875
- right_env: bfloat16 [768, 16, 256, 256], P('term', 'sector'), may hold values from -0.375 to 0.375
- target: int32 [768, 16], P('term', 'sector'), may hold values from 0 to 255, as said below
- source: int32 [768, 16], P('term', 'sector'), may hold values from 0 to 255, as said below
- live_count: int32 [16, 16], P('term', 'sector'), may hold values from 1 to 48, as said below
Outputs:
- sigma: float32 [256, 256, 256], P('sector', 'term')
The draws below stay inside these ranges and needn't reach their ends.
Inputs may be any that keep to these rules, and one draw needn't show every extreme that they name: target[j, g] lies among the sectors of sector group g, from g * 16 to (g + 1) * 16 - 1. source[j, g] differs from target[j, g] by at most 16. `live_count`: some device has all 48 slots live in every draw. `sector_sizes`: some sector has all 256 rows live in every draw.
All inputs are finite; a program needn't handle non-finite values.
Results may differ from the reference program's by a relative error of at most 0.0042.
Values may be sent and summed in bfloat16 or wider, within the bound.
No kernel may reach another device: no remote copies, remote signals or barrier semaphores. Data moves between devices by JAX's collectives and lax.ppermute only.
A program may use at most 128 MiB of HBM per device.

```python
import jax
import jax.numpy as jnp
from jax import lax

M = 256
SEC_DEV = 16
SLOT_DEV = 48
SECTORS = 256
GROUPS = 16
TGROUPS = 16
SLOTS = 768


def pair_plan(key):
    base = jax.random.fold_in(key, 7)
    offset = jax.random.randint(jax.random.fold_in(base, 1), (SLOTS, GROUPS), 0, SEC_DEV)
    groups_iota = jnp.arange(GROUPS, dtype=jnp.int32)[None, :]
    target_ids = (groups_iota * SEC_DEV + offset).astype(jnp.int32)
    moved = jax.random.randint(jax.random.fold_in(base, 2), (SLOTS, GROUPS), -SEC_DEV, SEC_DEV + 1)
    source_ids = jnp.clip(target_ids + moved, 0, SECTORS - 1).astype(jnp.int32)
    return (target_ids, source_ids)


def draw_target(key, part):
    return pair_plan(key)[0]


def draw_source(key, part):
    return pair_plan(key)[1]


def draw_live_count(key, part):
    base = jax.random.fold_in(key, 11)
    counts = jax.random.randint(jax.random.fold_in(base, 1), (TGROUPS * GROUPS,), 1, SLOT_DEV + 1)
    spot = jax.random.randint(jax.random.fold_in(base, 2), (), 0, TGROUPS * GROUPS)
    counts = jnp.where(jnp.arange(TGROUPS * GROUPS) == spot, SLOT_DEV, counts)
    return counts.reshape(TGROUPS, GROUPS).astype(jnp.int32)


def draw_sector_sizes(key, part):
    base = jax.random.fold_in(key, 13)
    sizes_drawn = jax.random.randint(jax.random.fold_in(base, 1), (SECTORS,), M // 4, M + 1)
    spot = jax.random.randint(jax.random.fold_in(base, 2), (), 0, SECTORS)
    sizes_drawn = jnp.where(jnp.arange(SECTORS) == spot, M, sizes_drawn)
    return sizes_drawn.astype(jnp.int32)


def levels(own_key, dims, pieces, least, top_value):
    level = 1.0
    for dim, parts in pieces:
        draws = jax.random.uniform(jax.random.fold_in(jax.random.fold_in(own_key, 6), dim), (parts,), jnp.float32, least / len(pieces), top_value / len(pieces))
        level = level * jnp.repeat(jnp.exp(draws), dims[dim] // parts).reshape((-1,) + (1,) * (len(dims) - 1 - dim))
    return level


def normal_values(own_key, shape, spread, most, shards=(), held_as=jnp.bfloat16):
    values = spread * jax.random.normal(own_key, shape, jnp.float32)
    if shards:
        values = values * levels(own_key, shape, shards, -0.22, 0.18)
    return jnp.clip(values, -most, most).astype(held_as)


def setup_inputs(seed: int = 0) -> dict:
    arg_keys = jax.random.split(jax.random.key(seed), 8)
    return {
        "psi": normal_values(arg_keys[0], (SECTORS, M, M), 1.0, 6.0, ((0, 16),)),
        "sector_sizes": draw_sector_sizes(jax.random.fold_in(arg_keys[7], 71), 0),
        "left_env": normal_values(arg_keys[2], (SLOTS, GROUPS, M, M), (M * SLOTS // SEC_DEV) ** -0.5, 0.0546875, ((0, 16), (1, 16))),
        "right_env": normal_values(arg_keys[3], (SLOTS, GROUPS, M, M), M ** -0.5, 0.375, ((0, 16), (1, 16))),
        "target": draw_target(jax.random.fold_in(arg_keys[7], 71), 0),
        "source": draw_source(jax.random.fold_in(arg_keys[7], 71), 0),
        "live_count": draw_live_count(jax.random.fold_in(arg_keys[7], 71), 0),
    }


def reference(psi, sector_sizes, left_env, right_env, target, source, live_count):
    index_row = jnp.arange(M, dtype=jnp.int32)
    keep = (index_row[None, :, None] < sector_sizes[:, None, None]) & (index_row[None, None, :] < sector_sizes[:, None, None])
    masked = jnp.where(keep, psi, jnp.zeros_like(psi))
    slot_ids = jnp.arange(SLOTS, dtype=jnp.int32)

    def visit(carry, inputs):
        left, right, tgt, src, slot = inputs
        picked = masked[src].astype(jnp.float32)
        inner = jnp.einsum("gab,gbc->gac", left.astype(jnp.float32), picked, precision=lax.Precision.HIGHEST).astype(jnp.bfloat16)
        contribution = jnp.einsum("gac,gdc->gad", inner.astype(jnp.float32), right.astype(jnp.float32), precision=lax.Precision.HIGHEST)
        alive = (slot % SLOT_DEV) < live_count[slot // SLOT_DEV]
        contribution = contribution * alive.astype(jnp.float32)[:, None, None]
        return carry.at[tgt].add(contribution), None

    start = jnp.zeros((SECTORS, M, M), jnp.float32)
    total, unused = lax.scan(visit, start, (left_env, right_env, target, source, slot_ids))
    return jnp.where(keep, total, jnp.zeros_like(total))
```

```python
import jax
import jax.numpy as jnp
from jax import lax
from jax.experimental import pallas as pl
from jax.experimental.pallas import tpu as pltpu
from jax.sharding import PartitionSpec as P


Z, CORES, Y, X = (8, 2, 4, 4)
BLOCK = 256
SECS = 16
SLOTS = 48
NOWHERE = -4096
SHARD = 3
DIRECT = SECS - 4 * SHARD
AXES = ("sector", "term")
HBM = pl.BlockSpec(memory_space=pltpu.HBM)
VMEM = pl.BlockSpec(memory_space=pltpu.VMEM)
SMEM = pl.BlockSpec(memory_space=pltpu.SMEM)
WIDTH = 6
CHUNK = 4
VLIM = 8 * 1024 * 1024


def device(z, core, y, x):
    return (z * CORES + core) * (Y * X) + y * X + x


def every():
    return [
        (z, core, y, x) for z in range(Z) for core in range(CORES) for y in range(Y) for x in range(X)
    ]


def partner_pairs():
    return [(device(z, c, y, x), device(z, 1 - c, y, x)) for z, c, y, x in every()]


def between_chips_pairs():
    return [
        (device(z, c, y, x), device(z + (1 if c else -1), 1 - c, y, x))
        for z, c, y, x in every()
        if 0 <= z + (1 if c else -1) < Z
    ]


def line_pairs(step, first):
    pairs = []
    for z, c, y, x in every():
        along_x = (c == 0) == first
        to = (y, (x + step) % X) if along_x else ((y + step) % Y, x)
        pairs.append((device(z, c, y, x), device(z, c, *to)))
    return pairs


def send(x, pairs):
    return lax.ppermute(x, AXES, pairs)


def place():
    sector = lax.axis_index("sector")
    term = lax.axis_index("term")
    return (sector, sector % CORES, term // X, term % X)


def blocks(n):
    return jax.ShapeDtypeStruct((n, BLOCK, BLOCK), jnp.bfloat16)


def masker():
    row = lax.broadcasted_iota(jnp.int32, (BLOCK, BLOCK), 0)
    col = lax.broadcasted_iota(jnp.int32, (BLOCK, BLOCK), 1)
    most = jnp.maximum(row, col)
    return lambda x, size: jnp.where(most < size, x.astype(jnp.float32), 0.0).astype(jnp.bfloat16)


def near_kernel(sizes_in, psi, near, buf, sizes, sems):
    get_sizes = pltpu.make_async_copy(sizes_in, sizes, sems.at[SHARD])
    get_sizes.start()
    _, core, y, x = place()
    c = jnp.where(core == 0, y, x)
    mask = masker()

    def fetch(i):
        return pltpu.make_async_copy(psi.at[c * SHARD + i], buf.at[i], sems.at[i])

    for i in range(SHARD):
        fetch(i).start()
    get_sizes.wait()
    for i in range(SHARD):
        fetch(i).wait()
        near[i] = mask(buf[i], sizes[c * SHARD + i])


def near_blocks(psi, sizes):
    return pl.pallas_call(
        near_kernel,
        in_specs=[HBM, HBM],
        out_specs=VMEM,
        out_shape=blocks(SHARD),
        scratch_shapes=[
            pltpu.VMEM((SHARD, BLOCK, BLOCK), jnp.bfloat16),
            pltpu.SMEM((SECS,), jnp.int32),
            pltpu.SemaphoreType.DMA((SHARD + 1,)),
        ],
        compiler_params=PARAMS,
        name="near_blocks",
    )(sizes, psi)


def prep_kernel(sizes_in, psi, masked, far, buf, sizes, sems):
    get_sizes = pltpu.make_async_copy(sizes_in, sizes, sems.at[SECS])
    get_sizes.start()
    _, core, y, x = place()
    c2 = (jnp.where(core == 0, y, x) + 2) % 4
    mask = masker()

    def fetch(k):
        return pltpu.make_async_copy(psi.at[k], buf.at[k], sems.at[k])

    for k in range(SECS):
        fetch(k).start()
    get_sizes.wait()

    def one(k, carry):
        fetch(k).wait()
        masked[k] = mask(buf[k], sizes[k])
        return carry

    lax.fori_loop(0, SECS, one, 0)
    for i in range(SHARD):
        far[i] = masked[c2 * SHARD + i]
    for i in range(DIRECT):
        far[SHARD + i] = masked[4 * SHARD + i]


def prep(psi, sizes):
    return pl.pallas_call(
        prep_kernel,
        in_specs=[HBM, HBM],
        out_specs=[VMEM] * 2,
        out_shape=[blocks(SECS), blocks(SHARD + DIRECT)],
        scratch_shapes=[
            pltpu.VMEM((SECS, BLOCK, BLOCK), jnp.bfloat16),
            pltpu.SMEM((SECS,), jnp.int32),
            pltpu.SemaphoreType.DMA((SECS + 1,)),
        ],
        compiler_params=PARAMS,
        name="prep",
    )(sizes, psi)


def listed(order, low, src):
    def collect(j, count):
        at = src[j] - low
        order[count] = j
        return count + ((at >= 0) & (at < SECS)).astype(jnp.int32)

    return lax.fori_loop(0, SLOTS, collect, jnp.int32(0))


def add_listed(order, count, low, tgt, src, lbuf, rbuf, wave, acc, ready):
    base = lax.axis_index("sector") * SECS

    def step(n, state):
        first = n * WIDTH
        state = ready(order[jnp.minimum(first + WIDTH, count) - 1], state)
        for u in range(WIDTH):
            there = first + u < count
            j = jnp.where(there, order[first + u], 0)
            s = jnp.where(there, src[j] - low, 0)
            t = jnp.where(there, tgt[j] - base, SECS)
            inner = jnp.dot(
                lbuf[j], wave[s], preferred_element_type=jnp.float32
            ).astype(jnp.bfloat16)
            acc[t] += lax.dot_general(
                inner, rbuf[j], (((1,), (1,)), ((), ())), preferred_element_type=jnp.float32
            )
        return state

    return lax.fori_loop(0, (count + WIDTH - 1) // WIDTH, step, jnp.int32(0))


def work_kernel(tgt, src, left, right, masked, partner, acc, lbuf, rbuf, lsem, rsem, order):
    sector, core, _, _ = place()


    def fetches(k):
        at = pl.ds(k * CHUNK, CHUNK)
        return (
            pltpu.make_async_copy(left.at[at, 0], lbuf.at[at], lsem.at[k]),
            pltpu.make_async_copy(right.at[at, 0], rbuf.at[at], rsem.at[k]),
        )

    for k in range(SLOTS // CHUNK):
        for copy in fetches(k):
            copy.start()

    own_low = sector * SECS
    partner_low = (sector + 1 - 2 * core) * SECS
    own_count = listed(order.at[0], own_low, src)
    partner_count = listed(order.at[1], partner_low, src)

    def zero(s, carry):
        acc[s] = jnp.zeros((BLOCK, BLOCK), jnp.float32)
        return carry

    lax.fori_loop(0, SECS, zero, 0)

    def wait(k, carry):
        for copy in fetches(k):
            copy.wait()
        return carry

    def ready(j, waited):
        need = jnp.maximum(j // CHUNK + 1, waited)
        lax.fori_loop(waited, need, wait, 0)
        return need

    waited = add_listed(order.at[0], own_count, own_low, tgt, src, lbuf, rbuf, masked, acc, ready)
    lax.fori_loop(waited, SLOTS // CHUNK, wait, 0)
    add_listed(
        order.at[1], partner_count, partner_low, tgt, src, lbuf, rbuf, partner, acc, lambda j, w: w
    )


def halo_kernel(
    tgt, src, sizes, lbuf, rbuf, own, plus, minus, far, before,
    acc, out_own, out_plus, out_minus, out_cross,
    wave, order,
):
    sector, core, y, x = place()
    c = jnp.where(core == 0, x, y)
    for ref, at in ((own, c), (plus, (c + 3) % 4), (minus, (c + 1) % 4), (far, (c + 2) % 4)):
        for i in range(SHARD):
            wave[at * SHARD + i] = ref[i]
    for i in range(DIRECT):
        wave[4 * SHARD + i] = far[SHARD + i]
    low = (sector - 1 + 2 * core) * SECS
    count = listed(order, low, src)
    add_listed(order, count, low, tgt, src, lbuf, rbuf, wave, acc, lambda j, w: w)

    q_rows = jnp.where(core == 0, 64, 16)
    c_rows = jnp.where(core == 0, 16, 64)
    row = lax.broadcasted_iota(jnp.int32, (16, BLOCK), 0)
    col = lax.broadcasted_iota(jnp.int32, (16, BLOCK), 1)

    def put(s, carry):
        size = sizes[s]
        for step, out in ((1, out_plus), (3, out_minus), (2, out_cross), (0, out_own)):
            to = (c + step) % 4
            for q in range(4):
                at = pl.multiple_of(q * q_rows + to * c_rows, 16)
                piece = acc[s, pl.ds(at, 16), :]
                kept = jnp.maximum(row + at, col) < size
                out[s, q] = jnp.where(kept, piece, 0.0).astype(jnp.bfloat16)
        return carry

    lax.fori_loop(0, SECS, put, 0)


def merge_kernel(own, plus, minus, cross, mine, to_plus, to_minus, to_cross):
    _, core, y, x = place()
    c = jnp.where(core == 0, y, x)

    def put(s, carry):
        for step, out in ((1, to_plus), (3, to_minus), (2, to_cross), (0, mine)):
            at = (c + step) % 4
            pieces = [ref[s, at].astype(jnp.float32) for ref in (own, plus, minus, cross)]
            out[s] = (pieces[0] + pieces[1] + (pieces[2] + pieces[3])).astype(out.dtype)
        return carry

    lax.fori_loop(0, SECS, put, 0)


def merge(*pieces):
    message = jax.ShapeDtypeStruct((SECS, 16, BLOCK), jnp.bfloat16)
    return pl.pallas_call(
        merge_kernel,
        in_specs=[VMEM] * 4,
        out_specs=[VMEM] * 4,
        out_shape=[jax.ShapeDtypeStruct((SECS, 16, BLOCK), jnp.float32)] + [message] * 3,
        compiler_params=PARAMS,
        name="merge",
    )(*pieces)


def last_kernel(mine, plus, minus, cross, out):
    pieces = [ref[...].astype(jnp.float32) for ref in (mine, plus, minus, cross)]
    out[...] = pieces[0] + pieces[1] + (pieces[2] + pieces[3])


def last_sum(*pieces):
    return pl.pallas_call(
        last_kernel,
        in_specs=[VMEM] * 4,
        out_specs=VMEM,
        out_shape=jax.ShapeDtypeStruct((SECS, 16, BLOCK), jnp.float32),
        compiler_params=PARAMS,
        name="last_sum",
    )(*pieces)


ACC = jax.ShapeDtypeStruct((SECS + 1, BLOCK, BLOCK), jnp.float32)
COST = pl.CostEstimate(flops=2 * 16 * 2 * BLOCK**3, bytes_accessed=16 * 4 * BLOCK * BLOCK, transcendentals=0)
PARAMS = pltpu.CompilerParams(vmem_limit_bytes=VLIM)


def work_slots(tgt, src, left, right, masked, partner):
    chunks = SLOTS // CHUNK
    return pl.pallas_call(
        work_kernel,
        in_specs=[SMEM] * 2 + [HBM] * 2 + [VMEM] * 2,
        out_specs=[VMEM] * 3,
        out_shape=[ACC, blocks(SLOTS), blocks(SLOTS)],
        scratch_shapes=[
            pltpu.SemaphoreType.DMA((chunks,)),
            pltpu.SemaphoreType.DMA((chunks,)),
            pltpu.SMEM((2, SLOTS + WIDTH), jnp.int32),
        ],
        compiler_params=PARAMS,
        cost_estimate=COST,
        name="work_slots",
    )(tgt, src, left, right, masked, partner)


def halo_slots(tgt, src, sizes, left, right, own, plus, minus, far, before):
    message = jax.ShapeDtypeStruct((SECS, 4, 16, BLOCK), jnp.bfloat16)
    return pl.pallas_call(
        halo_kernel,
        in_specs=[SMEM] * 3 + [VMEM] * 7,
        out_specs=[VMEM] * 5,
        out_shape=[ACC] + [message] * 4,
        scratch_shapes=[
            pltpu.VMEM((SECS, BLOCK, BLOCK), jnp.bfloat16),
            pltpu.SMEM((SLOTS + WIDTH,), jnp.int32),
        ],
        input_output_aliases={9: 0},
        compiler_params=PARAMS,
        cost_estimate=COST,
        name="halo_slots",
    )(tgt, src, sizes, left, right, own, plus, minus, far, before)


def on_device(psi, sector_sizes, left_env, right_env, target, source, live_count):
    target = target.reshape(SLOTS)
    alive = jnp.arange(SLOTS, dtype=jnp.int32) < live_count.reshape(1)
    source = jnp.where(alive, source.reshape(SLOTS), NOWHERE)
    left_env, right_env, psi, sizes = [
        pltpu.with_memory_space_constraint(v, pltpu.HBM)
        for v in (left_env, right_env, psi, sector_sizes)
    ]
    near = near_blocks(psi, sizes)
    near, psi = lax.optimization_barrier((near, psi))
    h_near = send(near, between_chips_pairs())
    masked, far = prep(psi, sizes)
    h_far = send(far, between_chips_pairs())
    from_partner = send(masked, partner_pairs())
    h_plus = send(h_near, line_pairs(1, True))
    h_minus = send(h_near, line_pairs(-1, True))
    total, left, right = work_slots(
        target, source, left_env, right_env, masked, from_partner
    )
    _, m_own, m_plus, m_minus, m_cross = halo_slots(
        target, source, sector_sizes, left, right,
        h_near, h_plus, h_minus, h_far, total,
    )
    g_cross = send(m_cross, line_pairs(2, True))
    g_plus = send(m_plus, line_pairs(1, True))
    g_minus = send(m_minus, line_pairs(-1, True))
    mine, s_plus, s_minus, s_cross = merge(m_own, g_plus, g_minus, g_cross)
    t_cross = send(s_cross, line_pairs(2, False))
    t_plus = send(s_plus, line_pairs(1, False))
    t_minus = send(s_minus, line_pairs(-1, False))
    return last_sum(mine, t_plus, t_minus, t_cross)


def solution(mesh):
    placed = (
        P("sector", None, None),
        P("sector"),
        P("term", "sector", None, None),
        P("term", "sector", None, None),
        P("term", "sector"),
        P("term", "sector"),
        P("term", "sector"),
    )
    return jax.shard_map(
        on_device, mesh=mesh, in_specs=placed, out_specs=P("sector", "term", None), check_vma=False
    )
```

```python
import jax
import jax.numpy as jnp
from jax import lax
from jax.experimental import pallas as pl
from jax.experimental.pallas import tpu as pltpu
from jax.sharding import PartitionSpec as P


Z, CORES, Y, X = (8, 2, 4, 4)
BLOCK = 256
SECS = 16
SLOTS = 48
SHARD = 3
DIRECT = SECS - 4 * SHARD
AXES = ("sector", "term")
HBM = pl.BlockSpec(memory_space=pltpu.HBM)
VMEM = pl.BlockSpec(memory_space=pltpu.VMEM)
SMEM = pl.BlockSpec(memory_space=pltpu.SMEM)
WIDTH = 8
HALO_WIDTH = 10
CHUNK = 4
VLIM = 7 * 1024 * 1024


def device(z, core, y, x):
    return (z * CORES + core) * (Y * X) + y * X + x


def every():
    return [
        (z, core, y, x) for z in range(Z) for core in range(CORES) for y in range(Y) for x in range(X)
    ]


def partner_pairs():
    return [(device(z, c, y, x), device(z, 1 - c, y, x)) for z, c, y, x in every()]


def between_chips_pairs():
    return [
        (device(z, c, y, x), device(z + (1 if c else -1), 1 - c, y, x))
        for z, c, y, x in every()
        if 0 <= z + (1 if c else -1) < Z
    ]


def line_pairs(step, first):
    pairs = []
    for z, c, y, x in every():
        along_x = (c == 0) == first
        to = (y, x ^ step) if along_x else (y ^ step, x)
        pairs.append((device(z, c, y, x), device(z, c, *to)))
    return pairs


def send(x, pairs):
    return lax.ppermute(x, AXES, pairs)


def place():
    sector = lax.axis_index("sector")
    term = lax.axis_index("term")
    return (sector, sector % CORES, term // X, term % X)


def blocks(n):
    return jax.ShapeDtypeStruct((n, BLOCK, BLOCK), jnp.bfloat16)


def masker():
    row = lax.broadcasted_iota(jnp.int32, (BLOCK, BLOCK), 0)
    col = lax.broadcasted_iota(jnp.int32, (BLOCK, BLOCK), 1)
    most = jnp.maximum(row, col)
    return lambda x, size: jnp.where(most < size, x.astype(jnp.float32), 0.0).astype(jnp.bfloat16)


def mask_all(sizes_in, psi, near, masked, far, buf, sizes, sems):
    get_sizes = pltpu.make_async_copy(sizes_in, sizes, sems.at[SECS])
    get_sizes.start()
    _, core, y, x = place()
    c = jnp.where(core == 0, y, x)
    c2 = c ^ 2
    mask = masker()

    def fetch(k):
        return pltpu.make_async_copy(psi.at[k], buf.at[k], sems.at[k])

    for k in range(SECS):
        fetch(k).start()
    get_sizes.wait()

    def one(k, carry):
        fetch(k).wait()
        masked[k] = mask(buf[k], sizes[k])
        return carry

    lax.fori_loop(0, SECS, one, 0)
    for i in range(SHARD):
        if near is not None:
            near[i] = masked[c * SHARD + i]
        far[i] = masked[c2 * SHARD + i]
    for i in range(DIRECT):
        far[SHARD + i] = masked[4 * SHARD + i]


def near_kernel(sizes_in, psi, near, masked, far, buf, sizes, sems):
    _, core, y, _ = place()

    @pl.when(core == 1)
    def _():
        mask_all(sizes_in, psi, near, masked, far, buf, sizes, sems)

    @pl.when(core == 0)
    def _():
        get_sizes = pltpu.make_async_copy(sizes_in, sizes, sems.at[SHARD])
        get_sizes.start()
        mask = masker()

        def fetch(i):
            return pltpu.make_async_copy(psi.at[y * SHARD + i], buf.at[i], sems.at[i])

        for i in range(SHARD):
            fetch(i).start()
        get_sizes.wait()
        for i in range(SHARD):
            fetch(i).wait()
            near[i] = mask(buf[i], sizes[y * SHARD + i])


def prep_kernel(sizes_in, psi, masked_in, far_in, masked, far, buf, sizes, sems):
    _, core, _, _ = place()

    @pl.when(core == 0)
    def _():
        mask_all(sizes_in, psi, None, masked, far, buf, sizes, sems)


def mask_scratch():
    return [
        pltpu.VMEM((SECS, BLOCK, BLOCK), jnp.bfloat16),
        pltpu.SMEM((SECS,), jnp.int32),
        pltpu.SemaphoreType.DMA((SECS + 1,)),
    ]


def near_blocks(psi, sizes):
    return pl.pallas_call(
        near_kernel,
        in_specs=[HBM] * 2,
        out_specs=[VMEM] * 3,
        out_shape=[blocks(SHARD), blocks(SECS), blocks(SHARD + DIRECT)],
        scratch_shapes=mask_scratch(),
        compiler_params=PARAMS,
        name="near_blocks",
    )(sizes, psi)


def prep(psi, sizes, masked, far):
    return pl.pallas_call(
        prep_kernel,
        in_specs=[HBM] * 2 + [VMEM] * 2,
        out_specs=[VMEM] * 2,
        out_shape=[blocks(SECS), blocks(SHARD + DIRECT)],
        scratch_shapes=mask_scratch(),
        input_output_aliases={2: 0, 3: 1},
        compiler_params=PARAMS,
        name="prep",
    )(sizes, psi, masked, far)


def listed(order, low, span, src, alive):
    def collect(j, count):
        at = src[j] - low
        order[count] = j
        return count + ((j < alive) & (at >= 0) & (at < span)).astype(jnp.int32)

    return lax.fori_loop(0, SLOTS, collect, jnp.int32(0), unroll=8)


def add_listed(width, order, count, low, tgt, src, lbuf, rbuf, wave, acc, ready):
    base = lax.axis_index("sector") * SECS

    def step(n, state):
        first = n * width
        state = ready(order[jnp.minimum(first + width, count) - 1], state)
        for u in range(width):
            there = first + u < count
            j = jnp.where(there, order[first + u], 0)
            s = jnp.where(there, src[j] - low, 0)
            t = jnp.where(there, tgt[j] - base, SECS)
            inner = jnp.dot(
                lbuf[j], wave[s], preferred_element_type=jnp.float32
            ).astype(jnp.bfloat16)
            acc[t] += lax.dot_general(
                inner, rbuf[j], (((1,), (1,)), ((), ())), preferred_element_type=jnp.float32
            )
        return state

    return lax.fori_loop(0, (count + width - 1) // width, step, jnp.int32(0))


def work_kernel(tgt, src, live, left, right, masked, partner, acc, lbuf, rbuf, wave, order, lsem, rsem):
    def fetches(k):
        at = pl.ds(k * CHUNK, CHUNK)
        return (
            pltpu.make_async_copy(left.at[at, 0], lbuf.at[at], lsem.at[k]),
            pltpu.make_async_copy(right.at[at, 0], rbuf.at[at], rsem.at[k]),
        )

    for k in range(SLOTS // CHUNK):
        for copy in fetches(k):
            copy.start()
    sector, core, _, _ = place()
    low = (sector - core) * SECS

    def fill(s, carry):
        acc[s] = jnp.zeros((BLOCK, BLOCK), jnp.float32)
        wave[core * SECS + s] = masked[s]
        wave[(1 - core) * SECS + s] = partner[s]
        return carry

    lax.fori_loop(0, SECS, fill, 0)
    count = listed(order, low, 2 * SECS, src, live[0, 0])

    def wait(k, carry):
        for copy in fetches(k):
            copy.wait()
        return carry

    def ready(j, waited):
        need = jnp.maximum(j // CHUNK + 1, waited)
        lax.fori_loop(waited, need, wait, 0)
        return need

    waited = add_listed(WIDTH, order, count, low, tgt, src, lbuf, rbuf, wave, acc, ready)
    lax.fori_loop(waited, SLOTS // CHUNK, wait, 0)


def halo_kernel(
    tgt, src, live, sizes, lbuf, rbuf, own, plus, minus, far, before,
    acc, out_own, out_plus, out_minus, out_cross,
    wave, order,
):
    sector, core, y, x = place()
    c = jnp.where(core == 0, x, y)
    for ref, at in ((own, c), (plus, c ^ 1), (minus, c ^ 3), (far, c ^ 2)):
        for i in range(SHARD):
            wave[at * SHARD + i] = ref[i]
    for i in range(DIRECT):
        wave[4 * SHARD + i] = far[SHARD + i]
    low = (sector - 1 + 2 * core) * SECS
    count = listed(order, low, SECS, src, live[0, 0])
    add_listed(HALO_WIDTH, order, count, low, tgt, src, lbuf, rbuf, wave, acc, lambda j, state: state)

    q_rows = jnp.where(core == 0, 64, 16)
    c_rows = jnp.where(core == 0, 16, 64)
    row = lax.broadcasted_iota(jnp.int32, (16, BLOCK), 0)
    col = lax.broadcasted_iota(jnp.int32, (16, BLOCK), 1)

    def put(s, carry):
        size = sizes[s]
        for step, out in ((1, out_plus), (3, out_minus), (2, out_cross), (0, out_own)):
            to = c ^ step
            for q in range(4):
                at = pl.multiple_of(q * q_rows + to * c_rows, 16)
                piece = acc[s, pl.ds(at, 16), :]
                kept = jnp.maximum(row + at, col) < size
                out[s, q] = jnp.where(kept, piece, 0.0).astype(jnp.bfloat16)
        return carry

    lax.fori_loop(0, SECS, put, 0)


def merge_kernel(own, plus, minus, cross, mine, to_plus, to_minus, to_cross):
    _, core, y, x = place()
    c = jnp.where(core == 0, y, x)

    def put(s, carry):
        for step, out in ((1, to_plus), (3, to_minus), (2, to_cross), (0, mine)):
            at = c ^ step
            pieces = [ref[s, at].astype(jnp.float32) for ref in (own, plus, minus, cross)]
            out[s] = (pieces[0] + pieces[1] + (pieces[2] + pieces[3])).astype(out.dtype)
        return carry

    lax.fori_loop(0, SECS, put, 0)


def merge(*pieces):
    message = jax.ShapeDtypeStruct((SECS, 16, BLOCK), jnp.bfloat16)
    return pl.pallas_call(
        merge_kernel,
        in_specs=[VMEM] * 4,
        out_specs=[VMEM] * 4,
        out_shape=[jax.ShapeDtypeStruct((SECS, 16, BLOCK), jnp.float32)] + [message] * 3,
        compiler_params=PARAMS,
        name="merge",
    )(*pieces)


def last_kernel(mine, plus, minus, cross, out):
    pieces = [ref[...].astype(jnp.float32) for ref in (mine, plus, minus, cross)]
    out[...] = pieces[0] + pieces[1] + (pieces[2] + pieces[3])


def last_sum(*pieces):
    return pl.pallas_call(
        last_kernel,
        in_specs=[VMEM] * 4,
        out_specs=VMEM,
        out_shape=jax.ShapeDtypeStruct((SECS, 16, BLOCK), jnp.float32),
        compiler_params=PARAMS,
        name="last_sum",
    )(*pieces)


ACC = jax.ShapeDtypeStruct((SECS + 1, BLOCK, BLOCK), jnp.float32)
COST = pl.CostEstimate(flops=2 * 16 * 2 * BLOCK**3, bytes_accessed=16 * 4 * BLOCK * BLOCK, transcendentals=0)
PARAMS = pltpu.CompilerParams(vmem_limit_bytes=VLIM)


def work_slots(tgt, src, live, left, right, masked, partner):
    return pl.pallas_call(
        work_kernel,
        in_specs=[SMEM] * 3 + [HBM] * 2 + [VMEM] * 2,
        out_specs=[VMEM] * 3,
        out_shape=[ACC, blocks(SLOTS), blocks(SLOTS)],
        scratch_shapes=[
            pltpu.VMEM((2 * SECS, BLOCK, BLOCK), jnp.bfloat16),
            pltpu.SMEM((SLOTS + 16,), jnp.int32),
            pltpu.SemaphoreType.DMA((SLOTS // CHUNK,)),
            pltpu.SemaphoreType.DMA((SLOTS // CHUNK,)),
        ],
        compiler_params=PARAMS,
        cost_estimate=COST,
        name="work_slots",
    )(tgt, src, live, left, right, masked, partner)


def halo_slots(tgt, src, live, sizes, left, right, own, plus, minus, far, before):
    message = jax.ShapeDtypeStruct((SECS, 4, 16, BLOCK), jnp.bfloat16)
    return pl.pallas_call(
        halo_kernel,
        in_specs=[SMEM] * 4 + [VMEM] * 7,
        out_specs=[VMEM] * 5,
        out_shape=[ACC] + [message] * 4,
        scratch_shapes=[
            pltpu.VMEM((SECS, BLOCK, BLOCK), jnp.bfloat16),
            pltpu.SMEM((SLOTS + 16,), jnp.int32),
        ],
        input_output_aliases={10: 0},
        compiler_params=PARAMS,
        cost_estimate=COST,
        name="halo_slots",
    )(tgt, src, live, sizes, left, right, own, plus, minus, far, before)


def on_device(psi, sector_sizes, left_env, right_env, target, source, live_count):
    target = target.reshape(SLOTS)
    source = source.reshape(SLOTS)
    live = jnp.pad(live_count, ((0, 7), (0, 127)))
    left_env, right_env, psi, sizes = [
        pltpu.with_memory_space_constraint(v, pltpu.HBM)
        for v in (left_env, right_env, psi, sector_sizes)
    ]
    near, masked, far = near_blocks(psi, sizes)
    h_near = send(near, between_chips_pairs())
    masked, far = prep(psi, sizes, masked, far)
    h_far = send(far, between_chips_pairs())
    from_partner = send(masked, partner_pairs())
    h_plus = send(h_near, line_pairs(1, True))
    h_minus = send(h_near, line_pairs(3, True))
    total, left, right = work_slots(target, source, live, left_env, right_env, masked, from_partner)
    _, m_own, m_plus, m_minus, m_cross = halo_slots(
        target, source, live, sector_sizes, left, right,
        h_near, h_plus, h_minus, h_far, total,
    )
    g_cross = send(m_cross, line_pairs(2, True))
    g_plus = send(m_plus, line_pairs(1, True))
    g_minus = send(m_minus, line_pairs(3, True))
    mine, s_plus, s_minus, s_cross = merge(m_own, g_plus, g_minus, g_cross)
    t_cross = send(s_cross, line_pairs(2, False))
    t_plus = send(s_plus, line_pairs(1, False))
    t_minus = send(s_minus, line_pairs(3, False))
    return last_sum(mine, t_plus, t_minus, t_cross)


def solution(mesh):
    placed = (
        P("sector", None, None),
        P("sector"),
        P("term", "sector", None, None),
        P("term", "sector", None, None),
        P("term", "sector"),
        P("term", "sector"),
        P("term", "sector"),
    )
    return jax.shard_map(
        on_device, mesh=mesh, in_specs=placed, out_specs=P("sector", "term", None), check_vma=False
    )
```

```python
import jax
import jax.numpy as jnp
from jax import lax
from jax.experimental import pallas as pl
from jax.experimental.pallas import tpu as pltpu
from jax.sharding import PartitionSpec as P


Z, CORES, Y, X = (8, 2, 4, 4)
BLOCK = 256
SECS = 16
SLOTS = 48
SHARD = 3
DIRECT = SECS - 4 * SHARD
AXES = ("sector", "term")
HBM = pl.BlockSpec(memory_space=pltpu.HBM)
VMEM = pl.BlockSpec(memory_space=pltpu.VMEM)
SMEM = pl.BlockSpec(memory_space=pltpu.SMEM)
WIDTH = 8
HALO_WIDTH = 10
CHUNK = 4
VLIM = 7 * 1024 * 1024


def device(z, core, y, x):
    return (z * CORES + core) * (Y * X) + y * X + x


def every():
    return [
        (z, core, y, x) for z in range(Z) for core in range(CORES) for y in range(Y) for x in range(X)
    ]


def partner_pairs():
    return [(device(z, c, y, x), device(z, 1 - c, y, x)) for z, c, y, x in every()]


def between_chips_pairs():
    return [
        (device(z, c, y, x), device(z + (1 if c else -1), 1 - c, y, x))
        for z, c, y, x in every()
        if 0 <= z + (1 if c else -1) < Z
    ]


def line_pairs(step, first):
    pairs = []
    for z, c, y, x in every():
        along_x = (c == 0) == first
        to = (y, x ^ step) if along_x else (y ^ step, x)
        pairs.append((device(z, c, y, x), device(z, c, *to)))
    return pairs


def send(x, pairs):
    return lax.ppermute(x, AXES, pairs)


def place():
    sector = lax.axis_index("sector")
    term = lax.axis_index("term")
    return (sector, sector % CORES, term // X, term % X)


def blocks(n):
    return jax.ShapeDtypeStruct((n, BLOCK, BLOCK), jnp.bfloat16)


def masker():
    row = lax.broadcasted_iota(jnp.int32, (BLOCK, BLOCK), 0)
    col = lax.broadcasted_iota(jnp.int32, (BLOCK, BLOCK), 1)
    most = jnp.maximum(row, col)
    return lambda x, size: jnp.where(most < size, x.astype(jnp.float32), 0.0).astype(jnp.bfloat16)


def mask_all(sizes_in, psi, near, masked, far, buf, sizes, sems):
    get_sizes = pltpu.make_async_copy(sizes_in, sizes, sems.at[SECS])
    get_sizes.start()
    _, core, y, x = place()
    c = jnp.where(core == 0, y, x)
    c2 = c ^ 2
    mask = masker()

    def fetch(k):
        return pltpu.make_async_copy(psi.at[k], buf.at[k], sems.at[k])

    for k in range(SECS):
        fetch(k).start()
    get_sizes.wait()

    def one(k, carry):
        fetch(k).wait()
        masked[k] = mask(buf[k], sizes[k])
        return carry

    lax.fori_loop(0, SECS, one, 0)
    for i in range(SHARD):
        if near is not None:
            near[i] = masked[c * SHARD + i]
        far[i] = masked[c2 * SHARD + i]
    for i in range(DIRECT):
        far[SHARD + i] = masked[4 * SHARD + i]


def near_kernel(sizes_in, psi, near, masked, far, buf, sizes, sems):
    _, core, y, _ = place()

    @pl.when(core == 1)
    def _():
        mask_all(sizes_in, psi, near, masked, far, buf, sizes, sems)

    @pl.when(core == 0)
    def _():
        get_sizes = pltpu.make_async_copy(sizes_in, sizes, sems.at[SHARD])
        get_sizes.start()
        mask = masker()

        def fetch(i):
            return pltpu.make_async_copy(psi.at[y * SHARD + i], buf.at[i], sems.at[i])

        for i in range(SHARD):
            fetch(i).start()
        get_sizes.wait()
        for i in range(SHARD):
            fetch(i).wait()
            near[i] = mask(buf[i], sizes[y * SHARD + i])


def prep_kernel(sizes_in, psi, masked_in, far_in, masked, far, buf, sizes, sems):
    _, core, _, _ = place()

    @pl.when(core == 0)
    def _():
        mask_all(sizes_in, psi, None, masked, far, buf, sizes, sems)


def mask_scratch():
    return [
        pltpu.VMEM((SECS, BLOCK, BLOCK), jnp.bfloat16),
        pltpu.SMEM((SECS,), jnp.int32),
        pltpu.SemaphoreType.DMA((SECS + 1,)),
    ]


def near_blocks(psi, sizes):
    return pl.pallas_call(
        near_kernel,
        in_specs=[HBM] * 2,
        out_specs=[VMEM] * 3,
        out_shape=[blocks(SHARD), blocks(SECS), blocks(SHARD + DIRECT)],
        scratch_shapes=mask_scratch(),
        compiler_params=PARAMS,
        name="near_blocks",
    )(sizes, psi)


def prep(psi, sizes, masked, far):
    return pl.pallas_call(
        prep_kernel,
        in_specs=[HBM] * 2 + [VMEM] * 2,
        out_specs=[VMEM] * 2,
        out_shape=[blocks(SECS), blocks(SHARD + DIRECT)],
        scratch_shapes=mask_scratch(),
        input_output_aliases={2: 0, 3: 1},
        compiler_params=PARAMS,
        name="prep",
    )(sizes, psi, masked, far)


def listed(order, low, span, src, alive):
    def collect(j, count):
        at = src[j] - low
        order[count] = j
        return count + ((j < alive) & (at >= 0) & (at < span)).astype(jnp.int32)

    return lax.fori_loop(0, SLOTS, collect, jnp.int32(0), unroll=8)


def add_listed(width, order, count, low, tgt, src, lbuf, rbuf, wave, acc, ready):
    base = lax.axis_index("sector") * SECS

    def step(n, state):
        first = n * width
        state = ready(order[jnp.minimum(first + width, count) - 1], state)
        for u in range(width):
            there = first + u < count
            j = jnp.where(there, order[first + u], 0)
            s = jnp.where(there, src[j] - low, 0)
            t = jnp.where(there, tgt[j] - base, SECS)
            inner = jnp.dot(
                lbuf[j], wave[s], preferred_element_type=jnp.float32
            ).astype(jnp.bfloat16)
            acc[t] += lax.dot_general(
                inner, rbuf[j], (((1,), (1,)), ((), ())), preferred_element_type=jnp.float32
            )
        return state

    return lax.fori_loop(0, (count + width - 1) // width, step, jnp.int32(0))


def work_kernel(
    tgt, src, live, sizes, left, right, masked, partner,
    acc, lbuf, rbuf, keep, wave, order, lsem, rsem,
):
    def fetches(k):
        at = pl.ds(k * CHUNK, CHUNK)
        return (
            pltpu.make_async_copy(left.at[at, 0], lbuf.at[at], lsem.at[k]),
            pltpu.make_async_copy(right.at[at, 0], rbuf.at[at], rsem.at[k]),
        )

    for k in range(SLOTS // CHUNK):
        for copy in fetches(k):
            copy.start()
    sector, core, _, _ = place()
    low = (sector - core) * SECS
    row = lax.broadcasted_iota(jnp.int32, (16, BLOCK), 0) + 16 * lax.axis_index("term")
    col = lax.broadcasted_iota(jnp.int32, (16, BLOCK), 1)
    most = jnp.maximum(row, col)

    def fill(s, carry):
        acc[s] = jnp.zeros((BLOCK, BLOCK), jnp.float32)
        wave[core * SECS + s] = masked[s]
        wave[(1 - core) * SECS + s] = partner[s]
        keep[s] = (most < sizes[s]).astype(jnp.float32)
        return carry

    lax.fori_loop(0, SECS, fill, 0)
    count = listed(order, low, 2 * SECS, src, live[0, 0])

    def wait(k, carry):
        for copy in fetches(k):
            copy.wait()
        return carry

    def ready(j, waited):
        need = jnp.maximum(j // CHUNK + 1, waited)
        lax.fori_loop(waited, need, wait, 0)
        return need

    waited = add_listed(WIDTH, order, count, low, tgt, src, lbuf, rbuf, wave, acc, ready)
    lax.fori_loop(waited, SLOTS // CHUNK, wait, 0)


def halo_kernel(
    tgt, src, live, lbuf, rbuf, own, plus, minus, far, before,
    acc, out_own, out_plus, out_minus, out_cross,
    wave, order,
):
    sector, core, y, x = place()
    c = jnp.where(core == 0, x, y)
    for ref, at in ((own, c), (plus, c ^ 1), (minus, c ^ 3), (far, c ^ 2)):
        for i in range(SHARD):
            wave[at * SHARD + i] = ref[i]
    for i in range(DIRECT):
        wave[4 * SHARD + i] = far[SHARD + i]
    low = (sector - 1 + 2 * core) * SECS
    count = listed(order, low, SECS, src, live[0, 0])
    add_listed(HALO_WIDTH, order, count, low, tgt, src, lbuf, rbuf, wave, acc, lambda j, state: state)

    q_rows = jnp.where(core == 0, 64, 16)
    c_rows = jnp.where(core == 0, 16, 64)

    def put(s, carry):
        for step, out in ((1, out_plus), (3, out_minus), (2, out_cross), (0, out_own)):
            to = c ^ step
            for q in range(4):
                at = pl.multiple_of(q * q_rows + to * c_rows, 16)
                out[s, q] = acc[s, pl.ds(at, 16), :].astype(jnp.bfloat16)
        return carry

    lax.fori_loop(0, SECS, put, 0)


def merge_kernel(own, plus, minus, cross, mine, to_plus, to_minus, to_cross):
    _, core, y, x = place()
    c = jnp.where(core == 0, y, x)

    def put(s, carry):
        for step, out in ((1, to_plus), (3, to_minus), (2, to_cross), (0, mine)):
            at = c ^ step
            pieces = [ref[s, at].astype(jnp.float32) for ref in (own, plus, minus, cross)]
            out[s] = (pieces[0] + pieces[1] + (pieces[2] + pieces[3])).astype(out.dtype)
        return carry

    lax.fori_loop(0, SECS, put, 0)


def merge(*pieces):
    message = jax.ShapeDtypeStruct((SECS, 16, BLOCK), jnp.bfloat16)
    return pl.pallas_call(
        merge_kernel,
        in_specs=[VMEM] * 4,
        out_specs=[VMEM] * 4,
        out_shape=[jax.ShapeDtypeStruct((SECS, 16, BLOCK), jnp.float32)] + [message] * 3,
        compiler_params=PARAMS,
        name="merge",
    )(*pieces)


def last_kernel(keep, mine, plus, minus, cross, out):
    pieces = [ref[...].astype(jnp.float32) for ref in (mine, plus, minus, cross)]
    total = pieces[0] + pieces[1] + (pieces[2] + pieces[3])
    out[...] = jnp.where(keep[...] > 0.0, total, 0.0)


def last_sum(*pieces):
    return pl.pallas_call(
        last_kernel,
        in_specs=[VMEM] * 5,
        out_specs=VMEM,
        out_shape=jax.ShapeDtypeStruct((SECS, 16, BLOCK), jnp.float32),
        compiler_params=PARAMS,
        name="last_sum",
    )(*pieces)


ROWS = jax.ShapeDtypeStruct((SECS, 16, BLOCK), jnp.float32)
ACC = jax.ShapeDtypeStruct((SECS + 1, BLOCK, BLOCK), jnp.float32)
COST = pl.CostEstimate(flops=2 * 16 * 2 * BLOCK**3, bytes_accessed=16 * 4 * BLOCK * BLOCK, transcendentals=0)
PARAMS = pltpu.CompilerParams(vmem_limit_bytes=VLIM)


def work_slots(tgt, src, live, sizes, left, right, masked, partner):
    return pl.pallas_call(
        work_kernel,
        in_specs=[SMEM] * 4 + [HBM] * 2 + [VMEM] * 2,
        out_specs=[VMEM] * 4,
        out_shape=[ACC, blocks(SLOTS), blocks(SLOTS), ROWS],
        scratch_shapes=[
            pltpu.VMEM((2 * SECS, BLOCK, BLOCK), jnp.bfloat16),
            pltpu.SMEM((SLOTS + 16,), jnp.int32),
            pltpu.SemaphoreType.DMA((SLOTS // CHUNK,)),
            pltpu.SemaphoreType.DMA((SLOTS // CHUNK,)),
        ],
        compiler_params=PARAMS,
        cost_estimate=COST,
        name="work_slots",
    )(tgt, src, live, sizes, left, right, masked, partner)


def halo_slots(tgt, src, live, left, right, own, plus, minus, far, before):
    message = jax.ShapeDtypeStruct((SECS, 4, 16, BLOCK), jnp.bfloat16)
    return pl.pallas_call(
        halo_kernel,
        in_specs=[SMEM] * 3 + [VMEM] * 7,
        out_specs=[VMEM] * 5,
        out_shape=[ACC] + [message] * 4,
        scratch_shapes=[
            pltpu.VMEM((SECS, BLOCK, BLOCK), jnp.bfloat16),
            pltpu.SMEM((SLOTS + 16,), jnp.int32),
        ],
        input_output_aliases={9: 0},
        compiler_params=PARAMS,
        cost_estimate=COST,
        name="halo_slots",
    )(tgt, src, live, left, right, own, plus, minus, far, before)


def on_device(psi, sector_sizes, left_env, right_env, target, source, live_count):
    target = target.reshape(SLOTS)
    source = source.reshape(SLOTS)
    live = jnp.pad(live_count, ((0, 7), (0, 127)))
    left_env, right_env, psi, sizes = [
        pltpu.with_memory_space_constraint(v, pltpu.HBM)
        for v in (left_env, right_env, psi, sector_sizes)
    ]
    near, masked, far = near_blocks(psi, sizes)
    h_near = send(near, between_chips_pairs())
    masked, far = prep(psi, sizes, masked, far)
    h_far = send(far, between_chips_pairs())
    from_partner = send(masked, partner_pairs())
    h_plus = send(h_near, line_pairs(1, True))
    h_minus = send(h_near, line_pairs(3, True))
    total, left, right, keep = work_slots(
        target, source, live, sector_sizes, left_env, right_env, masked, from_partner
    )
    _, m_own, m_plus, m_minus, m_cross = halo_slots(
        target, source, live, left, right,
        h_near, h_plus, h_minus, h_far, total,
    )
    g_cross = send(m_cross, line_pairs(2, True))
    g_plus = send(m_plus, line_pairs(1, True))
    g_minus = send(m_minus, line_pairs(3, True))
    mine, s_plus, s_minus, s_cross = merge(m_own, g_plus, g_minus, g_cross)
    t_cross = send(s_cross, line_pairs(2, False))
    t_plus = send(s_plus, line_pairs(1, False))
    t_minus = send(s_minus, line_pairs(3, False))
    return last_sum(keep, mine, t_plus, t_minus, t_cross)


def solution(mesh):
    placed = (
        P("sector", None, None),
        P("sector"),
        P("term", "sector", None, None),
        P("term", "sector", None, None),
        P("term", "sector"),
        P("term", "sector"),
        P("term", "sector"),
    )
    return jax.shard_map(
        on_device, mesh=mesh, in_specs=placed, out_specs=P("sector", "term", None), check_vma=False
    )
```
